32 devices in a mesh: seq: 16 (over z, y, core), tp: 2 (over x).
Axes of the slice: x: 2, y: 2, z: 4, core: 2. Of those that a mesh axis runs over, the one named last changes fastest.
Arguments:
- tokens: bfloat16 [16384, 1024], P('seq'), may hold values from -6 to 6
- cotangent: bfloat16 [16384, 1024], P('seq'), may hold values from -6 to 6
- mem_keys: bfloat16 [131072, 1024], P('seq', 'tp'), may hold values from -6 to 6
- mem_values: bfloat16 [131072, 1024], P('seq', 'tp'), may hold values from -6 to 6
- doc_ids: int32 [16, 1024], P('seq'), may hold values from 0 to 3, never falling along the last dimension, each value on 1 to 512 neighbouring positions
- mem_len: int32 [16], P('seq'), may hold values from 1 to 8192, 65536 in all
- owner_perm: int32 [32], replicated, may hold values from 0 to 31, each once
- gain_w: float32 [2, 1024], P(None, 'seq'), may hold values from 0.5 to 1.5
- gain_m: float32 [2, 1024], P(None, 'seq'), may hold values from -96 to 96
- gain_v: float32 [2, 1024], P(None, 'seq'), may hold values from 100 to 10000
- attn_w: float32 [4, 8, 32, 32, 128], P(None, 'tp', 'seq')
- attn_m: float32 [4, 8, 32, 32, 128], P(None, 'tp', 'seq')
- attn_v: float32 [4, 8, 32, 32, 128], P(None, 'tp', 'seq')
- attn_left: float32 [4, 8, 32, 32, 32], P(None, 'tp', 'seq')
- attn_right: float32 [4, 8, 32, 128, 128], P(None, 'tp', 'seq')
- mlp_w: float32 [3, 8, 32, 32, 352], P(None, 'tp', 'seq')
- mlp_m: float32 [3, 8, 32, 32, 352], P(None, 'tp', 'seq'), may hold values from -48 to 48
- mlp_v: float32 [3, 8, 32, 32, 352], P(None, 'tp', 'seq'), may hold values from 30 to 3000
- mlp_left: float32 [3, 8, 32, 32, 32], P(None, 'tp', 'seq')
- mlp_right: float32 [3, 8, 32, 352, 352], P(None, 'tp', 'seq')
Outputs:
- block_out: float32 [16384, 1024], P('seq')
- input_grad: float32 [16384, 1024], P('seq')
- new_keys: bfloat16 [16384, 1024], P('seq', 'tp')
- new_values: bfloat16 [16384, 1024], P('seq', 'tp')
- attn_grad: float32 [4, 8, 32, 32, 128], P(None, 'tp', 'seq')
- mlp_grad: float32 [3, 8, 32, 32, 352], P(None, 'tp', 'seq')
- gain_grad: float32 [2, 1024], P(None, 'seq')
- attn_update: float32 [4, 8, 32, 32, 128], P(None, 'tp', 'seq')
- attn_new_m: float32 [4, 8, 32, 32, 128], P(None, 'tp', 'seq')
- attn_new_v: float32 [3, 8, 32, 32, 128], P(None, 'tp', 'seq')
- out_new_v: float32 [8, 32, 32, 128], P('tp', 'seq')
- mlp_new_w: float32 [3, 8, 32, 32, 352], P(None, 'tp', 'seq')
- mlp_new_m: float32 [3, 8, 32, 32, 352], P(None, 'tp', 'seq')
- mlp_new_v: float32 [3, 8, 32, 32, 352], P(None, 'tp', 'seq')
- gain_update: float32 [2, 1024], P(None, 'seq')
- gain_new_m: float32 [2, 1024], P(None, 'seq')
- gain_new_v: float32 [2, 1024], P(None, 'seq')
The draws below stay inside these ranges and needn't reach their ends.
Inputs may be any that keep to these rules, and one draw needn't show every extreme that they name: `doc_ids`: document ids of each segment start at 0 and never fall along the segment. `mem_len`: live memory slots of each segment, the first ones of its cache. `owner_perm`: each row block number stands once.
All inputs are finite; a program needn't handle non-finite values. No bound on the sum of `mem_len` on one device may be relied on, other than what follows from the above.
Results may differ from the reference program's by a relative error of at most 0.018.
The reference program's roundings to bfloat16 on the way count: a program that leaves them out, or rounds other values in their place, can miss the bound.
Values may be sent and summed in bfloat16 or wider, within the bound.
A program may use at most 256 MiB of HBM per device.

```python
import math
import jax
import jax.numpy as jnp
import numpy as np
from jax import lax

D = 1024
H = 8
DH = 128
FF = 2816
FC = 352
BR = 32
SEG = 1024
MEM = 8192
TOKENS = 16384
NRB = 32
FG = 8
N_SEQ = 16


def near_identity(key, lead_shape, order):
    noise = jax.random.normal(key, lead_shape + (order, order), jnp.float32)
    return jnp.eye(order, dtype=jnp.float32) + 0.4 * order ** (-0.5) * noise


def draw_attn_w(key, part):
    noise = jax.random.normal(jax.random.fold_in(key, 3), (4, H, D // BR, BR, DH), jnp.float32)
    scales = jnp.array([D ** (-0.5), D ** (-0.5), D ** (-0.5), 0.5], jnp.float32)
    return noise * scales[:, None, None, None, None]


def draw_attn_m(key, part):
    noise = jax.random.normal(jax.random.fold_in(key, 19), (4, H, D // BR, BR, DH), jnp.float32)
    noise = jnp.clip(noise, -6.0, 6.0)
    scales = jnp.array([30.0, 30.0, 30.0, 6.0], jnp.float32)
    return noise * scales[:, None, None, None, None]


def draw_attn_v(key, part):
    unit = jax.random.uniform(jax.random.fold_in(key, 23), (4, H, D // BR, BR, DH), jnp.float32)
    lows = jnp.array([200.0, 200.0, 200.0, 5.0], jnp.float32)
    spread = jnp.log(200.0)
    return lows[:, None, None, None, None] * jnp.exp(spread * unit)


def draw_mlp_w(key, part):
    noise = jax.random.normal(jax.random.fold_in(key, 5), (3, FF // FC, D // BR, BR, FC), jnp.float32)
    scales = jnp.array([D ** (-0.5), D ** (-0.5), FF ** (-0.5)], jnp.float32)
    return noise * scales[:, None, None, None, None]


def draw_attn_left(key, part):
    return near_identity(jax.random.fold_in(key, 7), (4, H, D // BR), BR)


def draw_attn_right(key, part):
    return near_identity(jax.random.fold_in(key, 11), (4, H, D // BR), DH)


def draw_mlp_left(key, part):
    return near_identity(jax.random.fold_in(key, 13), (3, FF // FC, D // BR), BR)


def draw_mlp_right(key, part):
    return near_identity(jax.random.fold_in(key, 17), (3, FF // FC, D // BR), FC)


def block_scale(stream_key, shape, shards, smallest, top_value):
    def one(dim, shards_of):
        draws = jax.random.uniform(jax.random.fold_in(jax.random.fold_in(stream_key, 6), dim), (shards_of,), jnp.float32, smallest / len(shards), top_value / len(shards))
        return jnp.repeat(jnp.exp(draws), shape[dim] // shards_of).reshape((-1,) + (1,) * (len(shape) - dim - 1))

    factor_of = one(*shards[0])
    for cut in shards[1:]:
        factor_of = factor_of * one(*cut)
    return factor_of


def length_profile(number_of, total, bound, slope):
    portions = [(1 << 20) // math.isqrt(grade ** slope) + 1 for grade in range(2, number_of + 1)]
    surplus, given = total - bound - (number_of - 1), [1] * (number_of - 1)
    while surplus > 0:
        movable = [i for i in range(number_of - 1) if given[i] < bound]
        whole, budget = sum([portions[i] for i in movable]), surplus
        for i in movable:
            more = min(bound - given[i], max(1, budget * portions[i] // whole), surplus)
            given[i] = given[i] + more
            surplus = surplus - more
    return np.array([bound] + given)


def ragged_sizes(rng, number_of, total, most, skew):
    if number_of == 2:
        one = jax.random.randint(rng, (), max(1, total - most), min(most, total - 1) + 1)
        return jnp.stack([one, total - one])
    lengths = jnp.asarray(length_profile(number_of, total, most, skew), jnp.int32)
    twos = (number_of - 1) // 2
    source_of, receiver = lengths[1:1 + 2 * twos:2], lengths[2:2 + 2 * twos:2]
    room = jnp.minimum(source_of - 1, most - receiver)
    shifted = jax.random.randint(jax.random.fold_in(rng, 1), (twos,), 0, 1 << 20) % (room + 1)
    lengths = lengths.at[1:1 + 2 * twos:2].set(source_of - shifted).at[2:2 + 2 * twos:2].set(receiver + shifted)
    return lengths[jax.random.permutation(jax.random.fold_in(rng, 2), number_of)]


def centred(key, shape, scale, reach, shards=(), kind=jnp.bfloat16):
    gain = block_scale(key, shape, shards, -0.22, 0.18) if shards else 1.0
    values = jax.random.normal(key, shape, jnp.float32) * scale * gain
    return jnp.minimum(jnp.maximum(values, -reach), reach).astype(kind)


def setup_inputs(seed: int = 0) -> dict:
    splits = jax.random.split(jax.random.key(seed), 21)
    return {
        "tokens": centred(splits[0], (TOKENS, D), 1.0, 6.0, ((0, 16),)),
        "cotangent": centred(splits[1], (TOKENS, D), 1.0, 6.0, ((0, 16),)),
        "mem_keys": centred(splits[2], (N_SEQ * MEM, H * DH), 1.0, 6.0, ((0, 16), (1, 2))),
        "mem_values": centred(splits[3], (N_SEQ * MEM, H * DH), 1.0, 6.0, ((0, 16), (1, 2))),
        "doc_ids": jax.vmap(lambda own: jnp.searchsorted(jnp.cumsum(ragged_sizes(own, 4, SEG, SEG // 2, 2)), jnp.arange(SEG), side="right"))(jax.random.split(splits[4], N_SEQ)).reshape((N_SEQ, SEG)).astype(jnp.int32),
        "mem_len": ragged_sizes(splits[5], N_SEQ, N_SEQ * MEM // 2, MEM, 2).astype(jnp.int32),
        "owner_perm": jax.random.permutation(splits[6], NRB).astype(jnp.int32),
        "gain_w": jnp.clip(1.0 + 0.1 * jax.random.normal(splits[7], (2, D), jnp.float32), 0.5, 1.5),
        "gain_m": centred(splits[8], (2, D), 15.0, 96.0, ((1, 16),), jnp.float32),
        "gain_v": jnp.clip(jnp.exp(math.log(10000.0) - 4.6051702 * jax.random.uniform(splits[9], (2, D), jnp.float32) ** block_scale(splits[9], (2, D), ((1, 16),), -0.2, 0.2)), 100.0, 10000.0),
        "attn_w": draw_attn_w(jax.random.fold_in(splits[20], 71), 0),
        "attn_m": draw_attn_m(jax.random.fold_in(splits[20], 71), 0),
        "attn_v": draw_attn_v(jax.random.fold_in(splits[20], 71), 0),
        "attn_left": draw_attn_left(jax.random.fold_in(splits[20], 71), 0),
        "attn_right": draw_attn_right(jax.random.fold_in(splits[20], 71), 0),
        "mlp_w": draw_mlp_w(jax.random.fold_in(splits[20], 71), 0),
        "mlp_m": centred(splits[16], (3, FG, NRB, BR, FC), 8.0, 48.0, ((1, 2), (2, 16)), jnp.float32),
        "mlp_v": jnp.clip(jnp.exp(math.log(3000.0) - 4.6051702 * jax.random.uniform(splits[17], (3, FG, NRB, BR, FC), jnp.float32) ** block_scale(splits[17], (3, FG, NRB, BR, FC), ((1, 2), (2, 16)), -0.2, 0.2)), 30.0, 3000.0),
        "mlp_left": draw_mlp_left(jax.random.fold_in(splits[20], 71), 0),
        "mlp_right": draw_mlp_right(jax.random.fold_in(splits[20], 71), 0),
    }


@jax.custom_vjp
def low(v):
    return lax.optimization_barrier(v.astype(jnp.bfloat16)).astype(jnp.float32)

@jax.custom_vjp
def low_back(v):
    return v

def low_keep(v):
    return (low(v), None)

def low_pass(kept, grad):
    return (grad,)

def back_keep(v):
    return (v, None)

def back_low(kept, grad):
    return (low(grad),)
low.defvjp(low_keep, low_pass)
low_back.defvjp(back_keep, back_low)
norm_eps = 1e-06
adam_eps = 1e-08
beta_one = 0.9
beta_two = 0.95
learn_rate = 0.01
gain_rate = 0.02
corr_first = 1.0 - 0.9 ** 10
corr_second = 1.0 - 0.95 ** 10
masked_out = -1e+30
highest = lax.Precision.HIGHEST

def product(left_side, right_side):
    return jnp.dot(left_side, right_side, precision=highest, preferred_element_type=jnp.float32)

def to_matrix(blocks):
    groups, block_count, height, block_width = blocks.shape
    return jnp.transpose(blocks, (1, 2, 0, 3)).reshape(block_count * height, groups * block_width)

def rms_norm(values, gain_row):
    factor = lax.rsqrt(lax.optimization_barrier(jnp.mean(values * values, axis=-1, keepdims=True)) + norm_eps)
    return values * factor * gain_row

def head_attend(queries, keys_own, values_own, keys_memory, values_memory, doc_row, live_count):
    block_rows = min(512, SEG)
    keys_all = jnp.concatenate([keys_own, keys_memory], axis=0)
    values_all = jnp.concatenate([values_own, values_memory], axis=0)
    columns = jnp.arange(SEG, dtype=jnp.int32)
    memory_slots = jnp.arange(MEM, dtype=jnp.int32)

    def one_block(block_item):
        block_queries, start = block_item
        scores = low_back(product(block_queries, keys_all.T) * DH ** (-0.5))
        positions = start + jnp.arange(block_rows, dtype=jnp.int32)
        query_docs = lax.dynamic_slice_in_dim(doc_row, start, block_rows, 0)
        own_keep = (columns[None, :] <= positions[:, None]) & (doc_row[None, :] == query_docs[:, None])
        memory_keep = (memory_slots[None, :] < live_count) & (query_docs[:, None] == doc_row[0])
        keep_mask = jnp.concatenate([own_keep, memory_keep], axis=1)
        scores = jnp.where(keep_mask, scores, masked_out)
        row_top = lax.optimization_barrier(jnp.max(scores, axis=-1, keepdims=True))
        weights = jnp.exp(scores - row_top)
        softmax_rows = weights / lax.optimization_barrier(jnp.sum(weights, axis=-1, keepdims=True))
        return product(low(softmax_rows), values_all)
    starts = jnp.arange(SEG // block_rows, dtype=jnp.int32) * block_rows
    outputs = lax.map(jax.checkpoint(one_block), (queries.reshape(SEG // block_rows, block_rows, DH), starts))
    return outputs.reshape(SEG, DH)

def by_heads(array_in, length):
    return jnp.transpose(array_in.reshape(length, H, DH), (1, 0, 2))

def segment_forward(seg_tokens, gain_pair, weight_q, weight_k, weight_v, weight_o, weight_gate, weight_up, weight_down, keys_memory, values_memory, doc_row, live_count):
    normed = low(rms_norm(seg_tokens, gain_pair[0]))
    queries = low(low_back(product(normed, weight_q)))
    keys_new = low(low_back(product(normed, weight_k)))
    values_new = low(low_back(product(normed, weight_v)))

    def per_head(head_item):
        return head_attend(head_item[0], head_item[1], head_item[2], head_item[3], head_item[4], doc_row, live_count)
    head_outputs = lax.map(per_head, (by_heads(queries, SEG), by_heads(keys_new, SEG), by_heads(values_new, SEG), by_heads(keys_memory, MEM), by_heads(values_memory, MEM)))
    mixed_heads = low(low_back(jnp.transpose(head_outputs, (1, 0, 2)).reshape(SEG, H * DH)))
    hidden_state = seg_tokens + low_back(product(mixed_heads, weight_o))
    normed_two = low(rms_norm(hidden_state, gain_pair[1]))
    gate_val = low_back(product(normed_two, weight_gate))
    up_val = low_back(product(normed_two, weight_up))
    inner_act = low(jax.nn.silu(gate_val) * up_val)
    result = hidden_state + low_back(product(inner_act, weight_down))
    return (result, keys_new, values_new)

def forward_all(tokens_wide, gain_pair, attn_blocks, mlp_blocks, mem_keys, mem_values, doc_ids, mem_len):
    attn_low = low(attn_blocks)
    mlp_low = low(mlp_blocks)
    weight_q = to_matrix(attn_low[0])
    weight_k = to_matrix(attn_low[1])
    weight_v = to_matrix(attn_low[2])
    weight_o = to_matrix(attn_low[3]).T
    weight_gate = to_matrix(mlp_low[0])
    weight_up = to_matrix(mlp_low[1])
    weight_down = to_matrix(mlp_low[2]).T

    def one_segment(segment_item):
        seg_tokens, seg_keys, seg_values, doc_row, live_count = segment_item
        return segment_forward(seg_tokens, gain_pair, weight_q, weight_k, weight_v, weight_o, weight_gate, weight_up, weight_down, seg_keys.astype(jnp.float32), seg_values.astype(jnp.float32), doc_row, live_count)
    result, keys_new, values_new = lax.map(jax.checkpoint(one_segment), (tokens_wide.reshape(N_SEQ, SEG, D), mem_keys.reshape(N_SEQ, MEM, H * DH), mem_values.reshape(N_SEQ, MEM, H * DH), doc_ids, mem_len))
    return (result.reshape(N_SEQ * SEG, D), keys_new.reshape(N_SEQ * SEG, H * DH), values_new.reshape(N_SEQ * SEG, H * DH))

def rotate_step(grad, first, second, left_basis, right_basis):
    turned = jnp.einsum('...ji,...jk->...ik', left_basis, grad, precision=highest)
    turned = jnp.einsum('...ik,...kl->...il', turned, right_basis, precision=highest)
    first = beta_one * first + (1.0 - beta_one) * turned
    second = beta_two * second + (1.0 - beta_two) * turned * turned
    direction = first / corr_first / (jnp.sqrt(second / corr_second) + adam_eps)
    turned_back = jnp.einsum('...ij,...jk->...ik', left_basis, direction, precision=highest)
    turned_back = jnp.einsum('...ik,...lk->...il', turned_back, right_basis, precision=highest)
    return (-(learn_rate * turned_back), first, second)

def adam_step(grad, first, second):
    first = beta_one * first + (1.0 - beta_one) * grad
    second = beta_two * second + (1.0 - beta_two) * grad * grad
    direction = first / corr_first / (jnp.sqrt(second / corr_second) + adam_eps)
    return (-(gain_rate * direction), first, second)

def reference(tokens, cotangent, mem_keys, mem_values, doc_ids, mem_len, owner_perm, gain_w, gain_m, gain_v, attn_w, attn_m, attn_v, attn_left, attn_right, mlp_w, mlp_m, mlp_v, mlp_left, mlp_right):
    block_total = D // BR
    inverse = jnp.zeros((block_total,), jnp.int32).at[owner_perm].set(jnp.arange(block_total, dtype=jnp.int32))
    attn_blocks = attn_w[:, :, inverse]
    mlp_blocks = mlp_w[:, :, inverse]

    def forward(tokens_wide, gain_pair, attn_part, mlp_part):
        return forward_all(tokens_wide, gain_pair, attn_part, mlp_part, mem_keys, mem_values, doc_ids, mem_len)
    outcome, pullback = jax.vjp(forward, tokens.astype(jnp.float32), gain_w, attn_blocks, mlp_blocks)
    block_out, keys_new, values_new = outcome
    grad_tokens, grad_gain, grad_attn, grad_mlp = pullback((cotangent.astype(jnp.float32), jnp.zeros_like(keys_new), jnp.zeros_like(values_new)))
    attn_grad = grad_attn[:, :, owner_perm]
    mlp_grad = grad_mlp[:, :, owner_perm]
    attn_new = rotate_step(attn_grad, attn_m, attn_v, attn_left, attn_right)
    mlp_new = rotate_step(mlp_grad, mlp_m, mlp_v, mlp_left, mlp_right)
    gain_new = adam_step(grad_gain, gain_m, gain_v)
    return (block_out, grad_tokens, keys_new.astype(jnp.bfloat16), values_new.astype(jnp.bfloat16), attn_grad, mlp_grad, grad_gain, attn_new[0], attn_new[1], attn_new[2][:3], attn_new[2][3], mlp_w + mlp_new[0], mlp_new[1], mlp_new[2], gain_new[0], gain_new[1], gain_new[2])
```

```python
import functools
import math

import jax
import jax.numpy as jnp
from jax import lax
from jax.experimental import pallas as pl
from jax.experimental.pallas import tpu as pltpu
from jax.sharding import PartitionSpec as P

norm_eps = 1e-06
adam_eps = 1e-08
beta_one = 0.9
beta_two = 0.95
learn_rate = 0.01
gain_rate = 0.02
corr_first = 1.0 - 0.9**10
corr_second = 1.0 - 0.95**10
masked_out = -1e30
rotate_precision = lax.Precision.HIGH
row_tile = 256
f32 = jnp.float32
bf16 = jnp.bfloat16
grad_type = jnp.float32


def dot_nn(left, right):
    return lax.dot_general(left, right, (((1,), (0,)), ((), ())), preferred_element_type=f32)


def dot_nt(left, right):
    return lax.dot_general(left, right, (((1,), (1,)), ((), ())), preferred_element_type=f32)


def dot_tn(left, right):
    return lax.dot_general(left, right, (((0,), (0,)), ((), ())), preferred_element_type=f32)


def cost(flops, moved, exps=0):
    return pl.CostEstimate(flops=int(flops), bytes_accessed=int(moved), transcendentals=int(exps))


def own_mask(doc_rows, doc_cols, first_row, first_col):
    shape = (doc_rows.shape[0], doc_cols.shape[1])
    rows = first_row + lax.broadcasted_iota(jnp.int32, shape, 0)
    cols = first_col + lax.broadcasted_iota(jnp.int32, shape, 1)
    return (cols <= rows) & (doc_rows == doc_cols)


def own_windows(first_row, half):
    found = []
    for offset in range(0, half, row_tile):
        start = first_row + offset
        low_key = max(0, start - half)
        found.append((offset, low_key, start + row_tile - low_key))
    return found


def late_forward(half, coef, q_ref, k_ref, v_ref, dr_ref, dc_ref, o_ref, of_ref, lse_ref):
    for offset, low_key, keys in own_windows(half, half):
        rows = pl.ds(offset, row_tile)
        cols = pl.ds(low_key, keys)
        scores = dot_nt(q_ref[rows, :], k_ref[cols, :]) * coef
        keep = own_mask(dr_ref[rows, :], dc_ref[:, cols], half + offset, low_key)
        scores = jnp.where(keep, scores, masked_out)
        top = jnp.max(scores, axis=1, keepdims=True)
        weights = jnp.exp2(scores - top)
        total = jnp.sum(weights, axis=1, keepdims=True)
        out = dot_nn(weights.astype(bf16), v_ref[cols, :]) / total
        of_ref[rows, :] = out
        o_ref[rows, :] = out.astype(bf16)
        lse_ref[rows, :] = jnp.broadcast_to(top + jnp.log2(total), (row_tile, lse_ref.shape[1]))


def late_backward(
    half, coef, scale, q_ref, k_ref, v_ref, do_ref, of_ref, lse_ref, dr_ref, dc_ref,
    dq_ref, dk_ref, dv_ref, dk_low_ref, dv_low_ref, dk_sum, dv_sum,
):
    dk_sum[...] = jnp.zeros_like(dk_sum)
    dv_sum[...] = jnp.zeros_like(dv_sum)
    for offset, low_key, keys in own_windows(half, half):
        rows = pl.ds(offset, row_tile)
        cols = pl.ds(low_key, keys)
        own_backward(
            rows, cols, half + offset, low_key, coef, q_ref, k_ref, v_ref, do_ref, of_ref, lse_ref,
            dr_ref, dc_ref, dk_sum, dv_sum,
            lambda part: dq_ref.__setitem__((rows, slice(None)), (part * scale).astype(bf16)),
        )
    dk_low_ref[...] = dk_sum[pl.ds(0, half), :]
    dv_low_ref[...] = dv_sum[pl.ds(0, half), :]
    dk_ref[...] = (dk_sum[pl.ds(half, half), :] * scale).astype(bf16)
    dv_ref[...] = dv_sum[pl.ds(half, half), :].astype(bf16)


def own_backward(
    rows, cols, first_row, first_col, coef, q_ref, k_ref, v_ref, do_ref, of_ref, lse_ref,
    dr_ref, dc_ref, dk_sum, dv_sum, put_dq,
):
    q, do = q_ref[rows, :], do_ref[rows, :]
    k, v = k_ref[cols, :], v_ref[cols, :]
    scores = dot_nt(q, k) * coef
    keep = own_mask(dr_ref[rows, :], dc_ref[:, cols], first_row, first_col)
    weights = jnp.where(keep, jnp.exp2(jnp.where(keep, scores, masked_out) - lse_ref[rows, :1]), 0.0)
    delta = jnp.sum(do.astype(f32) * of_ref[rows, :], axis=1, keepdims=True)
    dscore = (weights * (dot_nt(do, v) - delta)).astype(bf16)
    put_dq(dot_nn(dscore, k))
    dk_sum[cols, :] += dot_tn(dscore, q)
    dv_sum[cols, :] += dot_tn(weights.astype(bf16), do)


def live_steps(live, step, block_keys, sub_keys):
    left = jnp.minimum(live - step * block_keys, block_keys)
    return left // sub_keys, left % sub_keys


def each_live(info_ref, step, block_keys, sub_keys, half, body):
    live, first_len = info_ref[0], info_ref[1]
    whole, rest = live_steps(live, step, block_keys, sub_keys)

    def tiles(sub, limit):
        for offset in range(0, half, row_tile):
            if offset == 0:
                body(offset, sub, limit)
            else:
                pl.when(first_len > offset)(functools.partial(body, offset, sub, limit))

    @pl.when(live > step * block_keys)
    def _():
        def full(sub, carry):
            tiles(sub, None)
            return carry

        lax.fori_loop(0, whole, full, 0)

        @pl.when(rest > 0)
        def _():
            tiles(whole, rest)


def early_forward(
    half, coef, block_keys, sub_keys, info_ref, q_ref, k_ref, v_ref, dr_ref, dc_ref, mk_ref, mv_ref,
    o_ref, of_ref, lse_ref, top_ref, total_ref, acc_ref,
):
    step = pl.program_id(1)

    @pl.when(step == 0)
    def _():
        for offset in range(0, half, row_tile):
            rows = pl.ds(offset, row_tile)
            cols = pl.ds(0, offset + row_tile)
            scores = dot_nt(q_ref[rows, :], k_ref[cols, :]) * coef
            keep = own_mask(dr_ref[rows, :], dc_ref[:, cols], offset, 0)
            scores = jnp.where(keep, scores, masked_out)
            top = jnp.max(scores, axis=1, keepdims=True)
            weights = jnp.exp2(scores - top)
            top_ref[rows, :] = jnp.broadcast_to(top, (row_tile, 128))
            total_ref[rows, :] = jnp.broadcast_to(
                jnp.sum(weights, axis=1, keepdims=True), (row_tile, 128)
            )
            acc_ref[rows, :] = dot_nn(weights.astype(bf16), v_ref[cols, :])

    def body(offset, sub, limit):
        rows = pl.ds(offset, row_tile)
        cols = pl.ds(pl.multiple_of(sub * sub_keys, sub_keys), sub_keys)
        sees = dr_ref[rows, :] == dr0(dc_ref)
        scores = dot_nt(q_ref[rows, :], mk_ref[cols, :]) * coef
        if limit is not None:
            slots = lax.broadcasted_iota(jnp.int32, (1, sub_keys), 1)
            scores = jnp.where(slots < limit, scores, masked_out)
        old_top = top_ref[rows, :1]
        new_top = jnp.where(
            sees, jnp.maximum(old_top, jnp.max(scores, axis=1, keepdims=True)), old_top
        )
        weights = jnp.exp2(scores - jnp.where(sees, new_top, -masked_out))
        fade = jnp.exp2(old_top - new_top)
        total_ref[rows, :] = total_ref[rows, :] * fade + jnp.sum(weights, axis=1, keepdims=True)
        acc_ref[rows, :] = acc_ref[rows, :] * fade + dot_nn(weights.astype(bf16), mv_ref[cols, :])
        top_ref[rows, :] = jnp.broadcast_to(new_top, (row_tile, 128))

    each_live(info_ref, step, block_keys, sub_keys, half, body)

    @pl.when(step == pl.num_programs(1) - 1)
    def _():
        total = total_ref[...]
        out = acc_ref[...] / total[:, :1]
        of_ref[...] = out
        o_ref[...] = out.astype(bf16)
        lse_ref[...] = top_ref[...] + jnp.log2(total)


def dr0(dc_ref):
    return dc_ref[:, :1]


def early_backward(
    half, coef, scale, block_keys, sub_keys, info_ref, q_ref, k_ref, v_ref, do_ref, of_ref, lse_ref,
    dr_ref, dc_ref, dk_low_ref, dv_low_ref, mk_ref, mv_ref, dq_ref, dk_ref, dv_ref,
    dq_sum, dk_sum, dv_sum, delta_ref,
):
    step = pl.program_id(1)

    @pl.when(step == 0)
    def _():
        dk_sum[...] = dk_low_ref[...]
        dv_sum[...] = dv_low_ref[...]
        for offset in range(0, half, row_tile):
            rows = pl.ds(offset, row_tile)
            cols = pl.ds(0, offset + row_tile)
            own_backward(
                rows, cols, offset, 0, coef, q_ref, k_ref, v_ref, do_ref, of_ref, lse_ref,
                dr_ref, dc_ref, dk_sum, dv_sum,
                lambda part: dq_sum.__setitem__((rows, slice(None)), part),
            )
            delta = jnp.sum(do_ref[rows, :].astype(f32) * of_ref[rows, :], axis=1, keepdims=True)
            delta_ref[rows, :] = jnp.broadcast_to(delta, (row_tile, 128))
        dk_ref[...] = (dk_sum[...] * scale).astype(bf16)
        dv_ref[...] = dv_sum[...].astype(bf16)

    def body(offset, sub, limit):
        rows = pl.ds(offset, row_tile)
        cols = pl.ds(pl.multiple_of(sub * sub_keys, sub_keys), sub_keys)
        sees = dr_ref[rows, :] == dr0(dc_ref)
        keys = mk_ref[cols, :]
        scores = dot_nt(q_ref[rows, :], keys) * coef
        if limit is not None:
            slots = lax.broadcasted_iota(jnp.int32, (1, sub_keys), 1)
            scores = jnp.where(slots < limit, scores, masked_out)
        weights = jnp.exp2(scores - jnp.where(sees, lse_ref[rows, :1], -masked_out))
        dprob = dot_nt(do_ref[rows, :], mv_ref[cols, :])
        dscore = (weights * (dprob - delta_ref[rows, :1])).astype(bf16)
        dq_sum[rows, :] += dot_nn(dscore, keys)

    each_live(info_ref, step, block_keys, sub_keys, half, body)

    @pl.when(step == pl.num_programs(1) - 1)
    def _():
        dq_ref[...] = (dq_sum[...] * scale).astype(bf16)


class Attention:
    def __init__(self, heads, size, seg_len, mem_rows):
        self.heads, self.size, self.seg_len, self.mem_rows = heads, size, seg_len, mem_rows
        self.half = seg_len // 2
        self.scale = size ** (-0.5)
        self.coef = self.scale * math.log2(math.e)
        self.block_keys = min(2048, mem_rows)
        self.sub_keys = min(1024, self.block_keys)
        self.steps = mem_rows // self.block_keys

    def late_specs(self):
        heads, size, half, seg = self.heads, self.size, self.half, self.seg_len
        return [
            pl.BlockSpec((half, size), lambda h: (1, h)),
            pl.BlockSpec((seg, size), lambda h: (0, heads + h)),
            pl.BlockSpec((seg, size), lambda h: (0, 2 * heads + h)),
        ]

    def doc_specs_late(self):
        return [
            pl.BlockSpec((self.half, 1), lambda h: (1, 0)),
            pl.BlockSpec((1, self.seg_len), lambda h: (0, 0)),
        ]

    def head_spec(self, grid_axes):
        if grid_axes == 1:
            return pl.BlockSpec((self.half, self.size), lambda h: (0, h))
        return pl.BlockSpec((self.half, self.size), lambda h, j, info: (0, h))

    def shape(self, dtype):
        return jax.ShapeDtypeStruct((self.half, self.heads * self.size), dtype)

    def forward_late(self, projected, doc_rows, doc_cols):
        head = self.head_spec(1)
        area = self.heads * self.half * self.half * 3
        return pl.pallas_call(
            functools.partial(late_forward, self.half, self.coef),
            grid=(self.heads,),
            in_specs=self.late_specs() + self.doc_specs_late(),
            out_specs=[head, head, head],
            out_shape=[self.shape(bf16), self.shape(f32), self.shape(f32)],
            cost_estimate=cost(area * 4 * self.size, 8 * 2**20, area),
            name="late_forward",
        )(projected, projected, projected, doc_rows, doc_cols)

    def backward_late(self, projected, do, of, lse, doc_rows, doc_cols):
        head = self.head_spec(1)
        area = self.heads * self.half * self.half * 3
        return pl.pallas_call(
            functools.partial(late_backward, self.half, self.coef, self.scale),
            grid=(self.heads,),
            in_specs=self.late_specs() + [head, head, head] + self.doc_specs_late(),
            out_specs=[head] * 5,
            out_shape=[self.shape(bf16)] * 3 + [self.shape(f32)] * 2,
            scratch_shapes=[pltpu.VMEM((self.seg_len, self.size), f32)] * 2,
            cost_estimate=cost(area * 10 * self.size, 12 * 2**20, area),
            name="late_backward",
        )(projected, projected, projected, do, of, lse, doc_rows, doc_cols)

    def early_specs(self):
        heads, size, half = self.heads, self.size, self.half
        return [
            pl.BlockSpec((half, size), lambda h, j, info: (0, h)),
            pl.BlockSpec((half, size), lambda h, j, info: (0, heads + h)),
            pl.BlockSpec((half, size), lambda h, j, info: (0, 2 * heads + h)),
        ]

    def doc_specs_early(self):
        return [
            pl.BlockSpec((self.half, 1), lambda h, j, info: (0, 0)),
            pl.BlockSpec((1, self.half), lambda h, j, info: (0, 0)),
        ]

    def memory_spec(self):
        block_keys = self.block_keys

        def index(h, j, info):
            return (jnp.minimum(j, (info[0] - 1) // block_keys), h)

        return pl.BlockSpec((block_keys, self.size), index)

    def forward_early(self, info, projected, doc_rows, doc_cols, mem_keys, mem_values):
        head = self.head_spec(2)
        memory = self.memory_spec()
        area = self.heads * self.half * self.mem_rows
        return pl.pallas_call(
            functools.partial(
                early_forward, self.half, self.coef, self.block_keys, self.sub_keys
            ),
            grid_spec=pltpu.PrefetchScalarGridSpec(
                num_scalar_prefetch=1,
                grid=(self.heads, self.steps),
                in_specs=self.early_specs() + self.doc_specs_early() + [memory, memory],
                out_specs=[head, head, head],
                scratch_shapes=[pltpu.VMEM((self.half, 128), f32)] * 2
                + [pltpu.VMEM((self.half, self.size), f32)],
            ),
            out_shape=[self.shape(bf16), self.shape(f32), self.shape(f32)],
            cost_estimate=cost(area * 4 * self.size, 24 * 2**20, area),
            name="early_forward",
        )(info, projected, projected, projected, doc_rows, doc_cols, mem_keys, mem_values)

    def backward_early(
        self, info, projected, do, of, lse, doc_rows, doc_cols, dk_low, dv_low, mem_keys, mem_values
    ):
        head = self.head_spec(2)
        memory = self.memory_spec()
        area = self.heads * self.half * self.mem_rows
        return pl.pallas_call(
            functools.partial(
                early_backward, self.half, self.coef, self.scale, self.block_keys, self.sub_keys
            ),
            grid_spec=pltpu.PrefetchScalarGridSpec(
                num_scalar_prefetch=1,
                grid=(self.heads, self.steps),
                in_specs=self.early_specs()
                + [head, head, head]
                + self.doc_specs_early()
                + [head, head, memory, memory],
                out_specs=[head] * 3,
                scratch_shapes=[pltpu.VMEM((self.half, self.size), f32)] * 3
                + [pltpu.VMEM((self.half, 128), f32)],
            ),
            out_shape=[self.shape(bf16)] * 3,
            cost_estimate=cost(area * 6 * self.size, 28 * 2**20, area),
            name="early_backward",
        )(
            info, projected, projected, projected, do, of, lse, doc_rows, doc_cols, dk_low, dv_low,
            mem_keys, mem_values,
        )


def mlp_body(
    parts, *refs
):
    x_ref, parts_refs, refs = refs[0], refs[1 : 1 + parts], refs[1 + parts :]
    (dy_ref, gain_ref, wg_ref, wu_ref, wd_ref,
     hs_ref, a2_ref, u_ref, dg_ref, du_ref, mlp_ref, da_ref) = refs
    branch = parts_refs[0][...].astype(f32)
    for other in parts_refs[1:]:
        branch = branch + other[...].astype(f32)
    hs = x_ref[...].astype(f32) + branch
    hs_ref[...] = hs
    factor = lax.rsqrt(jnp.mean(hs * hs, axis=1, keepdims=True) + norm_eps)
    a2 = (hs * factor * gain_ref[...]).astype(bf16)
    a2_ref[...] = a2
    dy = dy_ref[...]
    groups = wg_ref.shape[0]
    mlp = da = None
    for g in range(groups):
        gate = dot_nn(a2, wg_ref[g])
        up = dot_nn(a2, wu_ref[g])
        grad_inner = dot_nn(dy, wd_ref[g])
        sig = 1.0 / (1.0 + jnp.exp(-gate))
        silu = gate * sig
        inner = (silu * up).astype(bf16)
        dgate = (grad_inner * up * sig * (1.0 + gate * (1.0 - sig))).astype(bf16)
        dup = (grad_inner * silu).astype(bf16)
        u_ref[g] = inner
        dg_ref[g] = dgate
        du_ref[g] = dup
        mlp_g = dot_nt(inner, wd_ref[g])
        da_g = dot_nt(dgate, wg_ref[g]) + dot_nt(dup, wu_ref[g])
        mlp = mlp_g if mlp is None else mlp + mlp_g
        da = da_g if da is None else da + da_g
    mlp_ref[...] = mlp.astype(bf16)
    da_ref[...] = da.astype(bf16)


def mlp_both(x, parts, dy, first_block, gain_row, wg, wu, wd):
    groups, width, hidden = wg.shape
    rows = parts[0].shape[0]
    tile = min(row_tile, rows)
    base = first_block * (rows // tile)
    here = pl.BlockSpec((tile, width), lambda i: (i, 0))
    there = pl.BlockSpec((tile, width), lambda i: (base + i, 0))
    weight = pl.BlockSpec((groups, width, hidden), lambda i: (0, 0, 0), pipeline_mode=pl.Buffered(1))
    wide = pl.BlockSpec((groups, tile, hidden), lambda i: (0, i, 0))
    wide_shape = jax.ShapeDtypeStruct((groups, rows, hidden), bf16)
    return pl.pallas_call(
        functools.partial(mlp_body, len(parts)),
        grid=(rows // tile,),
        in_specs=[there]
        + [here] * len(parts)
        + [there, pl.BlockSpec((1, width), lambda i: (0, 0)), weight, weight, weight],
        out_specs=[here, here, wide, wide, wide, here, here],
        out_shape=[
            jax.ShapeDtypeStruct((rows, width), f32),
            jax.ShapeDtypeStruct((rows, width), bf16),
            wide_shape,
            wide_shape,
            wide_shape,
            jax.ShapeDtypeStruct((rows, width), bf16),
            jax.ShapeDtypeStruct((rows, width), bf16),
        ],
        cost_estimate=cost(12 * rows * width * hidden * groups, 24 * 2**20, rows * hidden * groups),
        name="mlp_both",
    )(x, *parts, dy, gain_row, wg, wu, wd)


def grad_body(kinds, steps, height, pack, *refs):
    out_ref = refs[-1]
    blocks, _, _, size = out_ref.shape
    for kind in range(kinds):

        @pl.when(pl.program_id(0) // steps == kind)
        def _():
            la, lb, ra, rb = refs[4 * kind : 4 * kind + 4]
            right = [r[0] if len(r.shape) == 3 else r[...] for r in (ra, rb)]
            total = dot_tn(la[...], right[0]) + dot_tn(lb[...], right[1])
            total = total.astype(grad_type)
            for i in range(pack):
                part = total[:, i * size : (i + 1) * size]
                out_ref[:, i] = part.reshape(blocks, height, size)


def grad_call(entries, height, size, name):
    kinds = len(entries)
    rows = entries[0][2][0].shape[-2]
    width = entries[0][0][0].shape[1]
    grouped = entries[0][2][0].ndim == 3
    if grouped:
        groups, pack = entries[0][2][0].shape[0], 1
    else:
        groups = entries[0][2][0].shape[1] // size
        pack = 2 if groups % 2 == 0 else 1
    steps = groups // pack
    specs, operands = [], []
    for kind, (left, left_blocks, right) in enumerate(entries):

        def place(g, kind=kind):
            return jnp.clip(g - kind * steps, 0, steps - 1)

        for half in range(2):
            specs.append(
                pl.BlockSpec(
                    (rows, width), lambda g, b=left_blocks[half]: (b, 0), pipeline_mode=pl.Buffered(1)
                )
            )
        for half in range(2):
            if grouped:
                specs.append(pl.BlockSpec((1, rows, size), lambda g, place=place: (place(g), 0, 0)))
            else:
                specs.append(pl.BlockSpec((rows, pack * size), lambda g, place=place: (0, place(g))))
        operands += [left[0], left[1], right[0], right[1]]
    return pl.pallas_call(
        functools.partial(grad_body, kinds, steps, height, pack),
        grid=(kinds * steps,),
        in_specs=specs,
        out_specs=pl.BlockSpec((width // height, pack, height, size), lambda g: (0, g, 0, 0)),
        out_shape=jax.ShapeDtypeStruct((width // height, kinds * groups, height, size), grad_type),
        cost_estimate=cost(4 * rows * width * size * groups * kinds, 16 * 2**20),
        name=name,
    )(*operands)


def to_matrix(blocks):
    groups, block_count, height, block_width = blocks.shape
    return jnp.transpose(blocks, (1, 2, 0, 3)).reshape(block_count * height, groups * block_width)


def rotate_step(grad, first, second, left_basis, right_basis):
    turned = jnp.einsum("...ji,...jk->...ik", left_basis, grad, precision=rotate_precision)
    turned = jnp.einsum("...ik,...kl->...il", turned, right_basis, precision=rotate_precision)
    first = beta_one * first + (1.0 - beta_one) * turned
    second = beta_two * second + (1.0 - beta_two) * turned * turned
    direction = first / corr_first / (jnp.sqrt(second / corr_second) + adam_eps)
    turned_back = jnp.einsum("...ij,...jk->...ik", left_basis, direction, precision=rotate_precision)
    turned_back = jnp.einsum(
        "...ik,...lk->...il", turned_back, right_basis, precision=rotate_precision
    )
    return (-(learn_rate * turned_back), first, second)


def adam_step(grad, first, second):
    first = beta_one * first + (1.0 - beta_one) * grad
    second = beta_two * second + (1.0 - beta_two) * grad * grad
    direction = first / corr_first / (jnp.sqrt(second / corr_second) + adam_eps)
    return (-(gain_rate * direction), first, second)


def norm_backward(values, gain_row, grad_normed):
    factor = lax.rsqrt(jnp.mean(values * values, axis=-1, keepdims=True) + norm_eps)
    scaled = grad_normed * gain_row
    inner_mean = jnp.mean(scaled * values, axis=-1, keepdims=True)
    grad_values = factor * scaled - values * (factor * factor * factor) * inner_mean
    grad_gain = jnp.sum(grad_normed * values * factor, axis=0)
    return (grad_values, grad_gain)


def back_to_order(values, one_hot):
    high = lax.reduce_precision(values, 8, 7)
    low = values - high
    return dot_nt(high.astype(bf16), one_hot) + dot_nt(low.astype(bf16), one_hot)


def on_device(
    tp_size,
    tokens,
    cotangent,
    mem_keys,
    mem_values,
    doc_ids,
    mem_len,
    owner_perm,
    gain_w,
    gain_m,
    gain_v,
    attn_w,
    attn_m,
    attn_v,
    attn_left,
    attn_right,
    mlp_w,
    mlp_m,
    mlp_v,
    mlp_left,
    mlp_right,
):
    def share(part):
        part = part.astype(bf16)
        if tp_size == 2:
            other = lax.ppermute(part, "tp", [(0, 1), (1, 0)])
            return [part, other]
        return [lax.psum(part, "tp")]

    def total(parts):
        out = parts[0].astype(f32)
        for other in parts[1:]:
            out = out + other.astype(f32)
        return out

    gain_stored = lax.all_gather(gain_w, "seq", axis=1, tiled=True)
    attn_low = lax.all_gather(attn_w.astype(bf16), "seq", axis=2, tiled=True)
    mlp_low = lax.all_gather(mlp_w.astype(bf16), "seq", axis=2, tiled=True)
    kinds, head_count, block_total, block_height, head_size = attn_low.shape
    group_count, hidden = mlp_low.shape[1], mlp_low.shape[4]
    seg_len, width = tokens.shape
    half = seg_len // 2
    width_heads = head_count * head_size

    order = (
        owner_perm[:, None] * block_height + jnp.arange(block_height, dtype=jnp.int32)[None, :]
    ).reshape(width)
    one_hot = (jnp.arange(width, dtype=jnp.int32)[:, None] == order[None, :]).astype(bf16)
    inverse = (
        jnp.zeros((block_total,), jnp.int32)
        .at[owner_perm]
        .set(jnp.arange(block_total, dtype=jnp.int32))
    )
    gain_pair = gain_stored.reshape(2, block_total, block_height)[:, owner_perm].reshape(2, width)
    x_low = dot_nn(tokens, one_hot).astype(bf16)
    dy_low = dot_nn(cotangent, one_hot).astype(bf16)

    doc_row = doc_ids
    doc_col = doc_ids.reshape(seg_len, 1)
    first_len = jnp.sum((doc_ids[0] == doc_ids[0, 0]).astype(jnp.int32))
    info = jnp.stack([mem_len[0], first_len]).astype(jnp.int32)
    attention = Attention(head_count, head_size, seg_len, mem_keys.shape[0])

    weight_qkv = jnp.concatenate([to_matrix(attn_low[i]) for i in range(3)], axis=1)
    weight_out = to_matrix(attn_low[3])
    mlp_mats = mlp_low.reshape(3, group_count, width, hidden)

    resid = x_low.astype(f32)
    factor_one = lax.rsqrt(jnp.mean(resid * resid, axis=-1, keepdims=True) + norm_eps)
    acts_one = (resid * factor_one * gain_pair[0]).astype(bf16)
    projected = dot_nn(acts_one, weight_qkv).astype(bf16)
    keys_new = projected[:, width_heads : 2 * width_heads]
    values_new = projected[:, 2 * width_heads :]

    o_late, of_late, lse_late = attention.forward_late(projected, doc_col, doc_row)
    attn_late = share(dot_nt(o_late, weight_out))
    o_early, of_early, lse_early = attention.forward_early(
        info, projected, doc_col, doc_row, mem_keys, mem_values
    )
    attn_early = share(dot_nt(o_early, weight_out))

    gain_two = gain_pair[1:2]
    hs_late, a2_late, u_late, dg_late, du_late, mlp_late, da_late = mlp_both(
        x_low, attn_late, dy_low, 1, gain_two, mlp_mats[0], mlp_mats[1], mlp_mats[2]
    )
    da_late = share(da_late)
    hs_early, a2_early, u_early, dg_early, du_early, mlp_early, da_early = mlp_both(
        x_low, attn_early, dy_low, 0, gain_two, mlp_mats[0], mlp_mats[1], mlp_mats[2]
    )
    da_early = share(da_early)
    mlp_late = share(mlp_late)
    mlp_early = share(mlp_early)

    def scatter(grads, kinds):
        owned = lax.psum_scatter(grads, "seq", scatter_dimension=0, tiled=True).astype(f32)
        own_blocks, _, height, size = owned.shape
        owned = owned.reshape(own_blocks, kinds, grads.shape[1] // kinds, height, size)
        return jnp.transpose(owned, (1, 2, 0, 3, 4))

    a2_pair = (a2_early, a2_late)
    mlp_grads = grad_call(
        [
            (a2_pair, (0, 0), (dg_early, dg_late)),
            (a2_pair, (0, 0), (du_early, du_late)),
            ((dy_low, dy_low), (0, 1), (u_early, u_late)),
        ],
        block_height,
        hidden,
        "mlp_grads",
    )
    mlp_grad = scatter(mlp_grads, 3)

    def hidden_grad(hs, dy, parts):
        grad, grad_gain = norm_backward(hs, gain_pair[1], total(parts))
        return dy.astype(f32) + grad, grad_gain

    dh_late, gain_late = hidden_grad(hs_late, dy_low[half:], da_late)
    dhr_late = dh_late.astype(bf16)
    do_late = dot_nn(dhr_late, weight_out).astype(bf16)
    dq_late, dk_late, dv_late, dk_low, dv_low = attention.backward_late(
        projected, do_late, of_late, lse_late, doc_col, doc_row
    )
    dproj_late = jnp.concatenate([dq_late, dk_late, dv_late], axis=1)
    one_late = share(dot_nt(dproj_late, weight_qkv))

    dh_early, gain_early = hidden_grad(hs_early, dy_low[:half], da_early)
    dhr_early = dh_early.astype(bf16)
    do_early = dot_nn(dhr_early, weight_out).astype(bf16)
    out_grads = grad_call(
        [((dhr_early, dhr_late), (0, 0), (o_early, o_late))], block_height, head_size, "out_grads"
    )
    out_grad = scatter(out_grads, 1)[0]
    dq_early, dk_early, dv_early = attention.backward_early(
        info, projected, do_early, of_early, lse_early, doc_col, doc_row, dk_low, dv_low,
        mem_keys, mem_values,
    )
    dproj_early = jnp.concatenate([dq_early, dk_early, dv_early], axis=1)
    one_early = share(dot_nt(dproj_early, weight_qkv))
    acts_pair = (acts_one, acts_one)
    qkv_grads = grad_call(
        [
            (acts_pair, (0, 1), (dq_early, dq_late)),
            (acts_pair, (0, 1), (dk_early, dk_late)),
            (acts_pair, (0, 1), (dv_early, dv_late)),
        ],
        block_height,
        head_size,
        "qkv_grads",
    )
    qkv_grad = scatter(qkv_grads, 3)
    attn_grad = jnp.concatenate([qkv_grad, out_grad[None]], axis=0)

    hidden_out = jnp.concatenate(
        [hs_early + total(mlp_early), hs_late + total(mlp_late)], axis=0
    )
    block_out = back_to_order(hidden_out, one_hot)

    grad_one = jnp.concatenate([total(one_early), total(one_late)], axis=0)
    grad_tokens, gain_first = norm_backward(resid, gain_pair[0], grad_one)
    grad_in = jnp.concatenate([dh_early, dh_late], axis=0) + grad_tokens
    input_grad = back_to_order(grad_in, one_hot)

    gain_grads = jnp.stack([gain_first, gain_early + gain_late])
    gain_grads = gain_grads.reshape(2, block_total, block_height)[:, inverse].reshape(2, width)
    gain_grad = lax.psum_scatter(gain_grads, "seq", scatter_dimension=1, tiled=True)

    mlp_new = rotate_step(mlp_grad, mlp_m, mlp_v, mlp_left, mlp_right)
    qkv_new = rotate_step(qkv_grad, attn_m[:3], attn_v[:3], attn_left[:3], attn_right[:3])
    out_new = rotate_step(out_grad, attn_m[3], attn_v[3], attn_left[3], attn_right[3])
    gain_new = adam_step(gain_grad, gain_m, gain_v)
    return (
        block_out,
        input_grad,
        keys_new,
        values_new,
        attn_grad,
        mlp_grad,
        gain_grad,
        jnp.concatenate([qkv_new[0], out_new[0][None]], axis=0),
        jnp.concatenate([qkv_new[1], out_new[1][None]], axis=0),
        qkv_new[2],
        out_new[2],
        mlp_w + mlp_new[0],
        mlp_new[1],
        mlp_new[2],
        gain_new[0],
        gain_new[1],
        gain_new[2],
    )


def solution(mesh):
    in_specs = (
        P("seq", None),
        P("seq", None),
        P("seq", "tp"),
        P("seq", "tp"),
        P("seq", None),
        P("seq"),
        P(),
        P(None, "seq"),
        P(None, "seq"),
        P(None, "seq"),
        P(None, "tp", "seq", None, None),
        P(None, "tp", "seq", None, None),
        P(None, "tp", "seq", None, None),
        P(None, "tp", "seq", None, None),
        P(None, "tp", "seq", None, None),
        P(None, "tp", "seq", None, None),
        P(None, "tp", "seq", None, None),
        P(None, "tp", "seq", None, None),
        P(None, "tp", "seq", None, None),
        P(None, "tp", "seq", None, None),
    )
    out_specs = (
        P("seq", None),
        P("seq", None),
        P("seq", "tp"),
        P("seq", "tp"),
        P(None, "tp", "seq", None, None),
        P(None, "tp", "seq", None, None),
        P(None, "seq"),
        P(None, "tp", "seq", None, None),
        P(None, "tp", "seq", None, None),
        P(None, "tp", "seq", None, None),
        P("tp", "seq", None, None),
        P(None, "tp", "seq", None, None),
        P(None, "tp", "seq", None, None),
        P(None, "tp", "seq", None, None),
        P(None, "seq"),
        P(None, "seq"),
        P(None, "seq"),
    )
    return jax.shard_map(
        functools.partial(on_device, mesh.shape["tp"]), mesh=mesh, in_specs=in_specs, out_specs=out_specs, check_vma=False
    )
```
